32 devices in a mesh: blk: 16 (over z, x, core), col: 2 (over y).
Axes of the slice: x: 2, y: 2, z: 4, core: 2. Of those that a mesh axis runs over, the one named last changes fastest.
Arguments:
- blocks: bfloat16 [16, 2, 2048, 2048], P('blk'), may hold values from -0.09375 to 0.09375
- offsets: int32 [16, 2], P('blk'), may hold values from -2 to 2, as said below
- krylov: bfloat16 [16, 64, 32768], P('col', None, 'blk'), may hold values from -6 to 6
- previous: float32 [64, 16, 32768], P(None, 'col', 'blk')
- node_table: float32 [32], replicated, may hold values from -1.5 to 1.5
- node_index: int32 [16], P('col'), may hold values from 0 to 31
- pole_values: float32 [16], P('col'), may hold values from 4 to 16
- scaling: float32 [16], P('col'), may hold values from 0.5 to 2
Outputs:
- new_basis: bfloat16 [16, 64, 32768], P('col', None, 'blk')
- first_coeffs: float32 [64, 64], replicated
- second_coeffs: float32 [64, 64], replicated
- factor: float32 [64, 64], replicated
The draws below stay inside these ranges and needn't reach their ends.
Inputs may be any that keep to these rules, and one draw needn't show every extreme that they name: `offsets`: each block row's 2 distances are distinct.
All inputs are finite; a program needn't handle non-finite values.
Results may differ from the reference program's by a relative error of at most 0.0012.
Values may be sent and summed in bfloat16 or wider, within the bound.
A program may use at most 128 MiB of HBM per device.

```python
import math
import jax
import jax.numpy as jnp
from jax import lax

BLOCK_ROWS = 2048
KRYLOV_COLS = 64
TERMS = 16
COUPLINGS = 2
REACH = 2
NODE_COUNT = 32
PREV_COLS = 64
ROWS = 32768
N_BLK = 16


def draw_offsets(key, part):
    width = 2 * REACH + 1
    scores = jax.random.randint(key, (N_BLK, width), 0, 1 << 20) * width + jnp.arange(width, dtype=jnp.int32)[None, :]
    chosen = lax.top_k(scores, COUPLINGS)[1]
    return (chosen - REACH).astype(jnp.int32)


def draw_previous(key, part):
    own_key = jax.random.fold_in(key, 11)
    common_key = jax.random.fold_in(key, 12)
    own = jax.random.normal(own_key, (PREV_COLS, TERMS, ROWS), jnp.float32)
    common = jax.random.normal(common_key, (1, TERMS, ROWS), jnp.float32)
    return (own + 0.125 * common).astype(jnp.float32)


def place_ends(array, stream_key, least, high):
    spot = [jax.random.randint(jax.random.fold_in(stream_key, axis), (), 0, length) for axis, length in enumerate(array.shape)]
    longest = array.shape.index(max(array.shape))
    next_to = spot[:longest] + [(spot[longest] + 1) % array.shape[longest]] + spot[longest + 1:]
    return array.at[tuple(spot)].set(least).at[tuple(next_to)].set(high)


def block_levels(rng, extent, split, low, high):
    factor_of = 1.0
    for axis_at, blocks in split:
        draws = jax.random.uniform(jax.random.fold_in(jax.random.fold_in(rng, 6), axis_at), (blocks,), jnp.float32, low / len(split), high / len(split))
        factor_of = factor_of * jnp.repeat(jnp.exp(draws), extent[axis_at] // blocks).reshape((-1,) + (1,) * (len(extent) - 1 - axis_at))
    return factor_of


def gaussian(rng, shape, scale, reach, cuts=(), kind=jnp.bfloat16):
    entries = scale * jax.random.normal(rng, shape, jnp.float32)
    if cuts:
        entries = entries * block_levels(rng, shape, cuts, -0.22, 0.18)
    return jnp.clip(entries, -reach, reach).astype(kind)


def setup_inputs(seed: int = 0) -> dict:
    arg_keys = jax.random.split(jax.random.key(seed), 9)
    blocks = gaussian(arg_keys[0], (N_BLK, COUPLINGS, BLOCK_ROWS, BLOCK_ROWS), (COUPLINGS * BLOCK_ROWS) ** -0.5, 0.09375, ((0, 16),))
    offsets = draw_offsets(jax.random.fold_in(arg_keys[8], 71), 0)
    krylov = gaussian(arg_keys[2], (TERMS, KRYLOV_COLS, ROWS), 1.0, 6.0, ((0, 2), (2, 16)))
    previous = draw_previous(jax.random.fold_in(arg_keys[8], 71), 0)
    node_table = jnp.clip(jax.random.uniform(arg_keys[4], (NODE_COUNT,), jnp.float32, -1.5, 1.5), -1.5, 1.5)
    node_index = place_ends(jax.random.randint(arg_keys[5], (TERMS,), 0, NODE_COUNT), jax.random.fold_in(arg_keys[5], 1), 0, NODE_COUNT - 1).astype(jnp.int32)
    pole_values = jnp.clip(jnp.exp(math.log(16.0) - 1.3862944 * jax.random.uniform(arg_keys[6], (TERMS,), jnp.float32) ** block_levels(arg_keys[6], (TERMS,), ((0, 2),), -0.2, 0.2)), 4.0, 16.0)
    scaling = jnp.clip(jnp.exp(math.log(2.0) - 1.3862944 * jax.random.uniform(arg_keys[7], (TERMS,), jnp.float32) ** block_levels(arg_keys[7], (TERMS,), ((0, 2),), -0.2, 0.2)), 0.5, 2.0)
    return {"blocks": blocks, "offsets": offsets, "krylov": krylov, "previous": previous, "node_table": node_table, "node_index": node_index, "pole_values": pole_values, "scaling": scaling}


exact_mode = lax.Precision.HIGHEST

def apply_band(blocks, offsets, krylov):
    flat = krylov.reshape(TERMS * KRYLOV_COLS, N_BLK, BLOCK_ROWS)

    def one_row(item):
        position, band, distances = item
        total = jnp.zeros((TERMS * KRYLOV_COLS, BLOCK_ROWS), jnp.float32)
        for coupling in range(COUPLINGS):
            source = ((position + distances[coupling]) % N_BLK).astype(jnp.int32)
            piece = lax.dynamic_index_in_dim(flat, source, 1, keepdims=False)
            total = total + lax.dot_general(piece.astype(jnp.float32), band[coupling].astype(jnp.float32), (((1,), (1,)), ((), ())), preferred_element_type=jnp.float32)
        return total
    image = lax.map(one_row, (jnp.arange(N_BLK, dtype=jnp.int32), blocks, offsets))
    return jnp.transpose(image, (1, 0, 2)).reshape(TERMS, KRYLOV_COLS, N_BLK * BLOCK_ROWS)

def reference(blocks, offsets, krylov, previous, node_table, node_index, pole_values, scaling):
    image = apply_band(blocks, offsets, krylov)
    matches = node_index[:, None] == jnp.arange(NODE_COUNT, dtype=jnp.int32)[None, :]
    shift_value = lax.optimization_barrier(jnp.sum(jnp.where(matches, node_table[None, :], jnp.float32(0.0)), axis=1))
    carry_weight = scaling / (1.0 - shift_value / pole_values)
    before = jnp.concatenate([jnp.zeros_like(krylov[:1]), krylov[:-1]], axis=0)
    work = image - shift_value[:, None, None] * krylov.astype(jnp.float32) + carry_weight[:, None, None] * before.astype(jnp.float32)
    inverse_size = 1.0 / (ROWS * TERMS)
    root_size = math.sqrt(ROWS * TERMS)
    coeff_one = jnp.einsum('ptn,tmn->pm', previous, work, precision=exact_mode) * inverse_size
    first_pass = work - jnp.einsum('ptn,pm->tmn', previous, coeff_one, precision=exact_mode)
    coeff_two = jnp.einsum('ptn,tmn->pm', previous, first_pass, precision=exact_mode) * inverse_size
    second_pass = first_pass - jnp.einsum('ptn,pm->tmn', previous, coeff_two, precision=exact_mode)
    gram = jnp.einsum('tkn,tmn->km', second_pass, second_pass, precision=exact_mode) * inverse_size
    factor = jnp.linalg.cholesky(gram)
    identity = jnp.eye(KRYLOV_COLS, dtype=jnp.float32)
    inverse_factor = jax.scipy.linalg.solve_triangular(factor, identity, lower=True)
    new_basis = jnp.einsum('tkn,mk->tmn', second_pass, inverse_factor, precision=exact_mode).astype(jnp.bfloat16)
    return (new_basis, coeff_one * root_size, coeff_two * root_size, factor)
```

```python
import functools
import math

import jax
import jax.numpy as jnp
from jax import lax
from jax.experimental import pallas as pl
from jax.experimental.pallas import tpu as pltpu
from jax.sharding import PartitionSpec as P

REACH = 2
WIDTH = 2 * REACH + 1
BF = jnp.bfloat16
F32 = jnp.float32
NT = (((1,), (1,)), ((), ()))
MESH = pl.DeviceIdType.MESH


def split(x):
    high = x.astype(BF)
    return high, (x - high.astype(F32)).astype(BF)


def dot_nt(a, b):
    return lax.dot_general(a, b, NT, preferred_element_type=F32)


def expand_kernel(
    n_blk, n_col, terms, cols, rows, groups,
    offsets, node_index, node_table, pole_values, scaling,
    krylov, blocks, previous,
    wst, pst, sums, last_sum, basis_sum,
    *scratch,
):
    bufs = scratch[:terms]
    (carry, band, prev, image, a_send, a_recv, b_send, b_recv, c_send, c_recv,
     d_send, d_recv, y_send, y_recv, own_sem, band_sem, prev_sem) = scratch[terms:]
    me = lax.axis_index("blk")
    col = lax.axis_index("col")
    core = lax.rem(me, 2)
    chip = lax.div(me, 2)
    par = lax.rem(chip, 2)
    n_chip = n_blk // 2
    n_prev = previous.shape[0]
    partner = (chip + 1 - 2 * par) * 2 + core
    ahead = lax.rem(chip + 2 - 4 * par + n_chip, n_chip) * 2 + core
    behind = lax.rem(chip - 2 + 4 * par + n_chip, n_chip) * 2 + core
    sibling = chip * 2 + 1 - core

    def remote(src, dst, send, recv, blk, colpos=None):
        return pltpu.make_async_remote_copy(
            src_ref=src, dst_ref=dst, send_sem=send, recv_sem=recv,
            device_id=(blk, col if colpos is None else colpos), device_id_type=MESH)

    own = [pltpu.make_async_copy(krylov.at[k], bufs[k].at[REACH], own_sem.at[k]) for k in range(terms)]
    band_copy = [pltpu.make_async_copy(blocks.at[0, c], band.at[c], band_sem.at[c]) for c in range(band.shape[0])]
    prev_copy = pltpu.make_async_copy(previous, prev, prev_sem)
    prev_copy.start()

    barrier = pltpu.get_barrier_semaphore()
    for blk in (partner, ahead, behind, sibling):
        pl.semaphore_signal(barrier, inc=1, device_id=(blk, col), device_id_type=MESH)
    if n_col > 1:
        for shift in (1, n_col - 1):
            pl.semaphore_signal(barrier, inc=1, device_id=(me, lax.rem(col + shift, n_col)), device_id_type=MESH)
    pl.semaphore_wait(barrier, 4 + (2 if n_col > 1 else 0))

    a_copy = [remote(krylov.at[k], bufs[k].at[4 * par], a_send.at[k], a_recv.at[k], partner) for k in range(terms)]
    c_copy = [remote(krylov.at[k], bufs[k].at[1 + 2 * core], c_send.at[k], c_recv.at[k], sibling) for k in range(terms)]
    b_copy = [remote(bufs[k].at[4 - 4 * par], bufs[k].at[4 * par], b_send.at[k], b_recv.at[k], ahead) for k in range(terms)]
    d_copy = [remote(bufs[k].at[4 - 4 * core], bufs[k].at[3 - 2 * core], d_send.at[k], d_recv.at[k], sibling) for k in range(terms)]
    y_copy = remote(krylov.at[terms - 1], carry, y_send, y_recv, me, lax.rem(col + 1, n_col))

    for k in range(terms):
        a_copy[k].start()
    for k in range(terms):
        c_copy[k].start()
    if n_col > 1:
        @pl.when(col < n_col - 1)
        def _():
            y_copy.start()
    for k in range(terms):
        own[k].start()
    for copy in band_copy:
        copy.start()

    @pl.when(col == 0)
    def _():
        carry[...] = jnp.zeros_like(carry)

    lane = 256

    def arrange(t):
        if t == 0:
            prev_copy.wait()
        p_at = t * 16

        def step(i, _):
            at = pl.ds(pl.multiple_of(i * lane, lane), lane)
            high, low = split(jnp.swapaxes(prev[p_at:p_at + 16, :, at], 0, 1))
            pst[:, p_at:p_at + 16, at] = high
            pst[:, n_prev + p_at:n_prev + p_at + 16, at] = low
            return 0
        lax.fori_loop(0, rows // lane, step, 0)

    def basis_term(t):
        part = dot_nt(pst[t], pst[t, :n_prev])
        if t == 0:
            basis_sum[...] = part
        else:
            basis_sum[...] += part

    tile = 256
    n_coupling = band.shape[0]

    def ready(group):
        for t in group:
            c_copy[t].wait_recv()
            d_copy[t].wait_recv()
            own[t].wait()
        if group[0] == 0:
            for copy in band_copy:
                copy.wait()

    def image_part(group, start, count):
        picks = [
            jnp.concatenate([bufs[t][offsets[0, c] + REACH] for t in group], axis=0)
            for c in range(n_coupling)
        ]

        def step(i, _):
            at = pl.ds(pl.multiple_of(i * tile, tile), tile)
            total = dot_nt(picks[0], band[0, at, :])
            for c in range(1, n_coupling):
                total = total + dot_nt(picks[c], band[c, at, :])
            image[group[0] * cols:(group[-1] + 1) * cols, at] = total
            return 0
        lax.fori_loop(start, start + count, step, 0)

    def finish(group):
        for t in group:
            shift = jnp.full((8, 128), node_table[node_index[t]], F32)
            weight = jnp.full((8, 128), scaling[t], F32) / (
                1.0 - shift / jnp.full((8, 128), pole_values[t], F32))
            before = carry if t == 0 else bufs[t - 1].at[REACH]
            if t == 0 and n_col > 1:
                @pl.when(col > 0)
                def _():
                    y_copy.wait_recv()
            work = (
                image[t * cols:(t + 1) * cols, :]
                - shift[:1, :1] * bufs[t][REACH].astype(F32)
                + weight[:1, :1] * before[...].astype(F32)
            )
            high, low = split(work)
            wst[t, :cols] = high
            wst[t, cols:] = low
            top = dot_nt(pst[t], high)
            self_part = dot_nt(wst[t], high)
            extra = dot_nt(pst[t, :n_prev], low)
            if t == 0:
                sums[:2 * n_prev] = top
                sums[2 * n_prev:] = self_part
                last_sum[...] = extra
            else:
                sums[:2 * n_prev] += top
                sums[2 * n_prev:] += self_part
                last_sum[...] += extra

    n_tiles = rows // tile
    plan = {}
    for j in range(n_prev // 16):
        plan.setdefault(j // 2, []).append(functools.partial(arrange, j))
    for t in range(terms):
        plan.setdefault(-(-n_prev // 32) + t // 3, []).append(functools.partial(basis_term, t))
    first = groups[0]
    begin = min(terms - 1, first[-1] + 2)
    plan.setdefault(begin, []).append(functools.partial(ready, first))
    left = terms - begin
    chunk = -(-n_tiles // left)
    for j in range(left):
        count = min(chunk, n_tiles - j * chunk)
        if count > 0:
            plan.setdefault(begin + j, []).append(functools.partial(image_part, first, j * chunk, count))

    for k in range(terms + 1):
        if k < terms:
            a_copy[k].wait_recv()
            b_copy[k].start()

            @pl.when(par == core)
            def _():
                d_copy[k].start()
        if k > 0:
            b_copy[k - 1].wait_recv()

            @pl.when(par != core)
            def _():
                d_copy[k - 1].start()
        for item in plan.get(k, ()):
            item()
    finish(first)
    for group in groups[1:]:
        ready(group)
        image_part(group, 0, n_tiles)
        finish(group)
    for k in range(terms):
        a_copy[k].wait_send()
        b_copy[k].wait_send()
        c_copy[k].wait_send()
        d_copy[k].wait_send()
    if n_col > 1:
        @pl.when(col < n_col - 1)
        def _():
            y_copy.wait_send()


def expand(n_blk, n_col, blocks, offsets, krylov, previous, node_table, node_index, pole_values, scaling):
    terms, cols, rows = krylov.shape
    n_prev = previous.shape[0]
    groups = (tuple(range(terms // 2)), tuple(range(terms // 2, 3 * terms // 4)), tuple(range(3 * terms // 4, terms)))
    smem = pl.BlockSpec(memory_space=pltpu.SMEM)
    hbm = pl.BlockSpec(memory_space=pl.ANY)
    vmem = pl.BlockSpec(memory_space=pltpu.VMEM)
    dma = pltpu.SemaphoreType.DMA
    return pl.pallas_call(
        functools.partial(expand_kernel, n_blk, n_col, terms, cols, rows, groups),
        out_shape=(
            jax.ShapeDtypeStruct((terms, 2 * cols, rows), BF),
            jax.ShapeDtypeStruct((terms, 2 * n_prev, rows), BF),
            jax.ShapeDtypeStruct((2 * n_prev + 2 * cols, cols), F32),
            jax.ShapeDtypeStruct((n_prev, cols), F32),
            jax.ShapeDtypeStruct((2 * n_prev, n_prev), F32),
        ),
        in_specs=[smem] * 5 + [hbm] * 3,
        out_specs=(vmem,) * 5,
        scratch_shapes=[pltpu.VMEM((WIDTH, cols, rows), BF)] * terms + [
            pltpu.VMEM((cols, rows), BF),
            pltpu.VMEM(blocks.shape[1:], BF),
            pltpu.VMEM(previous.shape, F32),
            pltpu.VMEM((terms * cols, rows), F32),
        ] + [dma((terms,))] * 8 + [dma, dma, dma((terms,)), dma((blocks.shape[1],)), dma],
        compiler_params=pltpu.CompilerParams(
            collective_id=0, has_side_effects=True, vmem_limit_bytes=60 * 1024 * 1024),
    )(offsets, node_index, node_table, pole_values, scaling,
      krylov, blocks, previous)


def final_kernel(inverse, mix, wst, pst, out):
    fh, fl = split(inverse[...])
    dh, dl = split(mix[...])
    half_w, half_p = fl.shape[1], dl.shape[1]
    total = jnp.dot(jnp.concatenate([fh, fh], 1), wst[0], preferred_element_type=F32)
    total += jnp.dot(jnp.concatenate([dh, dh], 1), pst[0], preferred_element_type=F32)
    total += jnp.dot(fl, wst[0, :half_w], preferred_element_type=F32)
    total += jnp.dot(dl, pst[0, :half_p], preferred_element_type=F32)
    out[0] = total.astype(BF)


def final(factor_inverse, mix, wst, pst):
    terms, _, rows = wst.shape
    cols = factor_inverse.shape[0]
    whole = pl.BlockSpec(memory_space=pltpu.VMEM)
    per_term = lambda a: pl.BlockSpec((1,) + a.shape[1:], lambda t: (t, 0, 0))
    return pl.pallas_call(
        final_kernel,
        grid=(terms,),
        out_shape=jax.ShapeDtypeStruct((terms, cols, rows), BF),
        in_specs=[whole] * 2 + [per_term(wst), per_term(pst)],
        out_specs=pl.BlockSpec((1, cols, rows), lambda t: (t, 0, 0)),
    )(factor_inverse, mix, wst, pst)


exact_mode = lax.Precision.HIGHEST


def exact(a, b):
    return jnp.dot(a, b, precision=exact_mode)


def body(n_blk, n_col, blocks, offsets, krylov, previous, node_table, node_index, pole_values, scaling):
    terms, cols, rows = krylov.shape
    n_prev = previous.shape[0]
    wst, pst, sums, last, basis = expand(
        n_blk, n_col, blocks, offsets, krylov, previous, node_table, node_index, pole_values, scaling)
    total_size = rows * n_blk * terms * n_col
    inverse_size = 1.0 / total_size
    root_size = math.sqrt(total_size)
    local_cross = (sums[:n_prev] + sums[n_prev:2 * n_prev] + last) * inverse_size
    low = sums[2 * n_prev + cols:]
    local_self = (sums[2 * n_prev:2 * n_prev + cols] + low + low.T) * inverse_size
    low = basis[n_prev:]
    local_basis = (basis[:n_prev] + low + low.T) * inverse_size
    cross, basis_gram, self_gram = lax.psum((local_cross, local_basis, local_self), ("blk", "col"))
    coeff_two = cross - exact(basis_gram, cross)
    combined = cross + coeff_two
    mixed = exact(combined.T, cross)
    gram = self_gram - mixed - mixed.T + exact(combined.T, exact(basis_gram, combined))
    factor = jnp.linalg.cholesky(gram)
    identity = jnp.eye(cols, dtype=F32)
    inverse_factor = jax.scipy.linalg.solve_triangular(factor, identity, lower=True)
    new_basis = final(inverse_factor, -exact(inverse_factor, combined.T), wst, pst)
    return (new_basis, cross * root_size, coeff_two * root_size, factor)


def solution(mesh):
    in_specs = (
        P("blk", None, None, None),
        P("blk", None),
        P("col", None, "blk"),
        P(None, "col", "blk"),
        P(),
        P("col"),
        P("col"),
        P("col"),
    )
    out_specs = (P("col", None, "blk"), P(), P(), P())
    call = functools.partial(body, mesh.shape["blk"], mesh.shape["col"])
    return jax.shard_map(call, mesh=mesh, in_specs=in_specs, out_specs=out_specs, check_vma=False)
```

```python
import functools
import math

import jax
import jax.numpy as jnp
from jax import lax
from jax.experimental import pallas as pl
from jax.experimental.pallas import tpu as pltpu
from jax.sharding import PartitionSpec as P

REACH = 2
WIDTH = 2 * REACH + 1
BF = jnp.bfloat16
F32 = jnp.float32
NT = (((1,), (1,)), ((), ()))
MESH = pl.DeviceIdType.MESH


def split(x):
    high = x.astype(BF)
    return high, (x - high.astype(F32)).astype(BF)


def dot_nt(a, b):
    return lax.dot_general(a, b, NT, preferred_element_type=F32)


def expand_kernel(
    n_blk, n_col, terms, cols, rows, groups,
    offsets, node_index, node_table, pole_values, scaling,
    krylov, blocks, previous,
    w_out, p_out, reduced,
    *scratch,
):
    bufs = scratch[:terms]
    (carry, band, prev, image, a_send, a_recv, b_send, b_recv, c_send, c_recv,
     d_send, d_recv, y_send, y_recv, own_sem, band_sem, prev_sem,
     wst, pst, sums, last_sum, basis_sum, part, rs_buf, z_buf, ag_buf,
     w_sem, p_sem, rs_send, rs_recv, z_send, z_recv, ag_send, ag_recv) = scratch[terms:]
    me = lax.axis_index("blk")
    col = lax.axis_index("col")
    core = lax.rem(me, 2)
    chip = lax.div(me, 2)
    par = lax.rem(chip, 2)
    n_chip = n_blk // 2
    n_prev = previous.shape[0]
    partner = (chip + 1 - 2 * par) * 2 + core
    ahead = lax.rem(chip + 2 - 4 * par + n_chip, n_chip) * 2 + core
    sibling = chip * 2 + 1 - core

    def remote(src, dst, send, recv, blk, colpos=None):
        return pltpu.make_async_remote_copy(
            src_ref=src, dst_ref=dst, send_sem=send, recv_sem=recv,
            device_id=(blk, col if colpos is None else colpos), device_id_type=MESH)

    own = [pltpu.make_async_copy(krylov.at[k], bufs[k].at[REACH], own_sem.at[k]) for k in range(terms)]
    band_copy = [pltpu.make_async_copy(blocks.at[0, c], band.at[c], band_sem.at[c]) for c in range(band.shape[0])]
    prev_copy = pltpu.make_async_copy(previous, prev, prev_sem)
    prev_copy.start()

    team, depth = part.shape[0], z_buf.shape[0]
    place = lax.rem(me, 4)
    layer = lax.div(me, 4)
    pos = place * n_col + col

    def member(j):
        other = lax.rem(pos + j, team)
        return other, layer * 4 + lax.div(other, n_col), lax.rem(other, n_col)

    def peer(j):
        return lax.rem(layer + j, depth) * 4 + place

    barrier = pltpu.get_barrier_semaphore()
    for j in range(1, team):
        _, blk, at_col = member(j)
        pl.semaphore_signal(barrier, inc=1, device_id=(blk, at_col), device_id_type=MESH)
    for j in range(1, depth):
        pl.semaphore_signal(barrier, inc=1, device_id=(peer(j), col), device_id_type=MESH)
    pl.semaphore_wait(barrier, team + depth - 2)

    a_copy = [remote(krylov.at[k], bufs[k].at[4 * par], a_send.at[k], a_recv.at[k], partner) for k in range(terms)]
    c_copy = [remote(krylov.at[k], bufs[k].at[1 + 2 * core], c_send.at[k], c_recv.at[k], sibling) for k in range(terms)]
    b_copy = [remote(bufs[k].at[4 - 4 * par], bufs[k].at[4 * par], b_send.at[k], b_recv.at[k], ahead) for k in range(terms)]
    d_copy = [remote(bufs[k].at[4 - 4 * core], bufs[k].at[3 - 2 * core], d_send.at[k], d_recv.at[k], sibling) for k in range(terms)]
    y_copy = remote(krylov.at[terms - 1], carry, y_send, y_recv, me, lax.rem(col + 1, n_col))

    for k in range(terms):
        a_copy[k].start()
    for k in range(terms):
        c_copy[k].start()
    if n_col > 1:
        @pl.when(col < n_col - 1)
        def _():
            y_copy.start()
    for k in range(terms):
        own[k].start()
    for copy in band_copy:
        copy.start()

    @pl.when(col == 0)
    def _():
        carry[...] = jnp.zeros_like(carry)

    w_copy = [pltpu.make_async_copy(wst.at[t], w_out.at[t], w_sem.at[t]) for t in range(terms)]
    p_copy = pltpu.make_async_copy(pst, p_out, p_sem)
    lane = 256

    def arrange(t):
        if t == 0:
            prev_copy.wait()
        p_at = t * 16

        def step(i, _):
            at = pl.ds(pl.multiple_of(i * lane, lane), lane)
            high, low = split(jnp.swapaxes(prev[p_at:p_at + 16, :, at], 0, 1))
            pst[:, p_at:p_at + 16, at] = high
            pst[:, n_prev + p_at:n_prev + p_at + 16, at] = low
            return 0
        lax.fori_loop(0, rows // lane, step, 0)
        if p_at + 16 == n_prev:
            p_copy.start()

    def basis_term(t):
        part = dot_nt(pst[t], pst[t, :n_prev])
        if t == 0:
            basis_sum[...] = part
        else:
            basis_sum[...] += part

    tile = 256
    n_coupling = band.shape[0]

    def ready(group):
        for t in group:
            c_copy[t].wait_recv()
            d_copy[t].wait_recv()
            own[t].wait()
        if group[0] == 0:
            for copy in band_copy:
                copy.wait()

    def image_part(group, start, count):
        picks = [
            jnp.concatenate([bufs[t][offsets[0, c] + REACH] for t in group], axis=0)
            for c in range(n_coupling)
        ]

        def step(i, _):
            at = pl.ds(pl.multiple_of(i * tile, tile), tile)
            total = dot_nt(picks[0], band[0, at, :])
            for c in range(1, n_coupling):
                total = total + dot_nt(picks[c], band[c, at, :])
            image[group[0] * cols:(group[-1] + 1) * cols, at] = total
            return 0
        lax.fori_loop(start, start + count, step, 0)

    def finish(group):
        for t in group:
            shift = jnp.full((8, 128), node_table[node_index[t]], F32)
            weight = jnp.full((8, 128), scaling[t], F32) / (
                1.0 - shift / jnp.full((8, 128), pole_values[t], F32))
            before = carry if t == 0 else bufs[t - 1].at[REACH]
            if t == 0 and n_col > 1:
                @pl.when(col > 0)
                def _():
                    y_copy.wait_recv()
            work = (
                image[t * cols:(t + 1) * cols, :]
                - shift[:1, :1] * bufs[t][REACH].astype(F32)
                + weight[:1, :1] * before[...].astype(F32)
            )
            high, low = split(work)
            wst[t, :cols] = high
            wst[t, cols:] = low
            w_copy[t].start()
            top = dot_nt(pst[t], high)
            self_part = dot_nt(wst[t], high)
            extra = dot_nt(pst[t, :n_prev], low)
            if t == 0:
                sums[:2 * n_prev] = top
                sums[2 * n_prev:] = self_part
                last_sum[...] = extra
            else:
                sums[:2 * n_prev] += top
                sums[2 * n_prev:] += self_part
                last_sum[...] += extra

    n_tiles = rows // tile
    plan = {}
    for j in range(n_prev // 16):
        plan.setdefault(j // 2, []).append(functools.partial(arrange, j))
    for t in range(terms):
        plan.setdefault(-(-n_prev // 32) + t // 3, []).append(functools.partial(basis_term, t))
    first = groups[0]
    begin = min(terms - 1, first[-1] + 2)
    plan.setdefault(begin, []).append(functools.partial(ready, first))
    left = terms - begin
    chunk = -(-n_tiles // left)
    for j in range(left):
        count = min(chunk, n_tiles - j * chunk)
        if count > 0:
            plan.setdefault(begin + j, []).append(functools.partial(image_part, first, j * chunk, count))

    for k in range(terms + 1):
        if k < terms:
            a_copy[k].wait_recv()
            b_copy[k].start()

            @pl.when(par == core)
            def _():
                d_copy[k].start()
        if k > 0:
            b_copy[k - 1].wait_recv()

            @pl.when(par != core)
            def _():
                d_copy[k - 1].start()
        for item in plan.get(k, ()):
            item()
    finish(first)
    for group in groups[1:]:
        ready(group)
        image_part(group, 0, n_tiles)
        finish(group)
    low = sums[2 * n_prev + cols:]
    head = jnp.concatenate([
        sums[:n_prev] + sums[n_prev:2 * n_prev] + last_sum[...],
        sums[2 * n_prev:2 * n_prev + cols] + low + low.T,
    ], axis=1)
    low = basis_sum[n_prev:]
    basis = basis_sum[:n_prev] + low + low.T
    full = jnp.concatenate([head, jnp.concatenate([basis, jnp.zeros_like(basis)], axis=1)], axis=0)
    part[...] = full.reshape(part.shape)
    copies = []
    for j in range(1, team):
        other, blk, at_col = member(j)
        copies.append(remote(part.at[other], rs_buf.at[j - 1], rs_send.at[j - 1], rs_recv.at[j - 1], blk, at_col))
        copies[-1].start()
    total = part[pos]
    for j, copy in enumerate(copies):
        copy.wait_recv()
        total = total + rs_buf[j]
    z_buf[layer] = total
    z_copies = [
        remote(z_buf.at[layer], z_buf.at[layer], z_send.at[j - 1], z_recv.at[j - 1], peer(j))
        for j in range(1, depth)]
    for copy in z_copies:
        copy.start()
    for copy in z_copies:
        copy.wait_recv()
    total = z_buf[0]
    for j in range(1, depth):
        total = total + z_buf[j]
    ag_buf[pos] = total
    ag_copies = []
    for j in range(1, team):
        _, blk, at_col = member(j)
        ag_copies.append(remote(ag_buf.at[pos], ag_buf.at[pos], ag_send.at[j - 1], ag_recv.at[j - 1], blk, at_col))
        ag_copies[-1].start()
    for k in range(terms):
        a_copy[k].wait_send()
        b_copy[k].wait_send()
        c_copy[k].wait_send()
        d_copy[k].wait_send()
        w_copy[k].wait()
    p_copy.wait()
    if n_col > 1:
        @pl.when(col < n_col - 1)
        def _():
            y_copy.wait_send()
    for copy in ag_copies:
        copy.wait_recv()
    reduced[...] = ag_buf[...].reshape(reduced.shape)
    for copy in copies + z_copies + ag_copies:
        copy.wait_send()


def expand(n_blk, n_col, blocks, offsets, krylov, previous, node_table, node_index, pole_values, scaling):
    terms, cols, rows = krylov.shape
    n_prev = previous.shape[0]
    groups = (tuple(range(terms // 2)), tuple(range(terms // 2, 3 * terms // 4)), tuple(range(3 * terms // 4, terms)))
    smem = pl.BlockSpec(memory_space=pltpu.SMEM)
    hbm = pl.BlockSpec(memory_space=pl.ANY)
    vmem = pl.BlockSpec(memory_space=pltpu.VMEM)
    dma = pltpu.SemaphoreType.DMA
    team, depth = 4 * n_col, n_blk // 4
    height = cols + n_prev
    piece = (height // team, 2 * cols)
    return pl.pallas_call(
        functools.partial(expand_kernel, n_blk, n_col, terms, cols, rows, groups),
        out_shape=(
            jax.ShapeDtypeStruct((terms, 2 * cols, rows), BF),
            jax.ShapeDtypeStruct((terms, 2 * n_prev, rows), BF),
            jax.ShapeDtypeStruct((height, 2 * cols), F32),
        ),
        in_specs=[smem] * 5 + [hbm] * 3,
        out_specs=(hbm, hbm, vmem),
        scratch_shapes=[pltpu.VMEM((WIDTH, cols, rows), BF)] * terms + [
            pltpu.VMEM((cols, rows), BF),
            pltpu.VMEM(blocks.shape[1:], BF),
            pltpu.VMEM(previous.shape, F32),
            pltpu.VMEM((terms * cols, rows), F32),
        ] + [dma((terms,))] * 8 + [dma, dma, dma((terms,)), dma((blocks.shape[1],)), dma] + [
            pltpu.VMEM((terms, 2 * cols, rows), BF),
            pltpu.VMEM((terms, 2 * n_prev, rows), BF),
            pltpu.VMEM((2 * n_prev + 2 * cols, cols), F32),
            pltpu.VMEM((n_prev, cols), F32),
            pltpu.VMEM((2 * n_prev, n_prev), F32),
            pltpu.VMEM((team,) + piece, F32),
            pltpu.VMEM((team - 1,) + piece, F32),
            pltpu.VMEM((depth,) + piece, F32),
            pltpu.VMEM((team,) + piece, F32),
            dma((terms,)), dma,
            dma((team - 1,)), dma((team - 1,)),
            dma((depth - 1,)), dma((depth - 1,)),
            dma((team - 1,)), dma((team - 1,)),
        ],
        compiler_params=pltpu.CompilerParams(
            collective_id=0, has_side_effects=True, vmem_limit_bytes=60 * 1024 * 1024),
    )(offsets, node_index, node_table, pole_values, scaling,
      krylov, blocks, previous)


def exact(a, b):
    return jnp.dot(a, b, precision=lax.Precision.HIGHEST, preferred_element_type=F32)


def final_kernel(total_size, reduced, w_in, p_in, out, first, second, factor, stack, result, in_sem, out_sem):
    terms, depth, rows = stack.shape
    cols = first.shape[1]
    n_prev = first.shape[0]
    w_copy = [pltpu.make_async_copy(w_in.at[t], stack.at[t, pl.ds(0, 2 * cols)], in_sem.at[0, t]) for t in range(terms)]
    p_copy = [pltpu.make_async_copy(p_in.at[t], stack.at[t, pl.ds(2 * cols, 2 * n_prev)], in_sem.at[1, t]) for t in range(terms)]
    for t in range(terms):
        w_copy[t].start()
        p_copy[t].start()
    inverse_size = 1.0 / total_size
    root_size = math.sqrt(total_size)
    cross = reduced[:n_prev, :cols] * inverse_size
    self_gram = reduced[:n_prev, cols:] * inverse_size
    basis_gram = reduced[n_prev:, :n_prev] * inverse_size
    coeff_two = cross - exact(basis_gram, cross)
    combined = cross + coeff_two
    turned = combined.T
    mixed = exact(turned, cross)
    gram = self_gram - mixed - mixed.T + exact(turned, exact(basis_gram, combined))
    first[...] = cross * root_size
    second[...] = coeff_two * root_size
    row = lax.broadcasted_iota(jnp.int32, (cols, cols), 0)
    lane = lax.broadcasted_iota(jnp.int32, (cols, cols), 1)
    both = jnp.concatenate([gram, jnp.where(row == lane, 1.0, 0.0)], axis=1)
    below = lax.broadcasted_iota(jnp.int32, (cols, 1), 0)
    for k in range(cols - 1):
        ratio = jnp.where(below > k, both[:, k:k + 1] * (1.0 / both[k:k + 1, k:k + 1]), 0.0)
        both = both - ratio * both[k:k + 1, :]
    left, right = both[:, :cols], both[:, cols:]
    pivots = jnp.sum(jnp.where(row == lane, left, 0.0), axis=1, keepdims=True)
    scale = 1.0 / jnp.sqrt(pivots)
    factor[...] = jnp.where(lane >= row, left * scale, 0.0).T
    inverse = jnp.where(lane <= row, right * scale, 0.0)
    mix = -exact(inverse, turned)
    fh, fl = split(inverse)
    dh, dl = split(mix)
    zero_f, zero_d = jnp.zeros_like(fl), jnp.zeros_like(dl)
    weights = jnp.concatenate([
        jnp.concatenate([fh, fh, dh, dh], axis=1),
        jnp.concatenate([fl, zero_f, dl, zero_d], axis=1),
    ], axis=0)
    out_copy = [pltpu.make_async_copy(result.at[t], out.at[t], out_sem.at[t]) for t in range(terms)]
    for t in range(terms):
        w_copy[t].wait()
        p_copy[t].wait()
        both = jnp.dot(weights, stack[t], preferred_element_type=F32)
        result[t] = (both[:cols] + both[cols:]).astype(BF)
        out_copy[t].start()
    for t in range(terms):
        out_copy[t].wait()


def final(total_size, reduced, wst, pst):
    terms, _, rows = wst.shape
    cols, n_prev = wst.shape[1] // 2, pst.shape[1] // 2
    vmem = pl.BlockSpec(memory_space=pltpu.VMEM)
    hbm = pl.BlockSpec(memory_space=pl.ANY)
    small = jax.ShapeDtypeStruct((n_prev, cols), F32)
    dma = pltpu.SemaphoreType.DMA
    return pl.pallas_call(
        functools.partial(final_kernel, total_size),
        out_shape=(jax.ShapeDtypeStruct((terms, cols, rows), BF), small, small, jax.ShapeDtypeStruct((cols, cols), F32)),
        in_specs=[vmem, hbm, hbm],
        out_specs=(hbm, vmem, vmem, vmem),
        scratch_shapes=[
            pltpu.VMEM((terms, 2 * cols + 2 * n_prev, rows), BF),
            pltpu.VMEM((terms, cols, rows), BF),
            dma((2, terms)), dma((terms,)),
        ],
        compiler_params=pltpu.CompilerParams(vmem_limit_bytes=40 * 1024 * 1024),
    )(reduced, wst, pst)


def body(n_blk, n_col, blocks, offsets, krylov, previous, node_table, node_index, pole_values, scaling):
    terms, cols, rows = krylov.shape
    wst, pst, reduced = expand(
        n_blk, n_col, blocks, offsets, krylov, previous, node_table, node_index, pole_values, scaling)
    return final(rows * n_blk * terms * n_col, reduced, wst, pst)


def solution(mesh):
    in_specs = (
        P("blk", None, None, None),
        P("blk", None),
        P("col", None, "blk"),
        P(None, "col", "blk"),
        P(),
        P("col"),
        P("col"),
        P("col"),
    )
    out_specs = (P("col", None, "blk"), P(), P(), P())
    call = functools.partial(body, mesh.shape["blk"], mesh.shape["col"])
    return jax.shard_map(call, mesh=mesh, in_specs=in_specs, out_specs=out_specs, check_vma=False)
```

```python
import functools
import math

import jax
import jax.numpy as jnp
from jax import lax
from jax.experimental import pallas as pl
from jax.experimental.pallas import tpu as pltpu
from jax.sharding import PartitionSpec as P

REACH = 2
WIDTH = 2 * REACH + 1
BF = jnp.bfloat16
F32 = jnp.float32
NT = (((1,), (1,)), ((), ()))
MESH = pl.DeviceIdType.MESH


def split(x):
    high = x.astype(BF)
    return high, (x - high.astype(F32)).astype(BF)


def dot_nt(a, b):
    return lax.dot_general(a, b, NT, preferred_element_type=F32)


def expand_kernel(
    n_blk, n_col, terms, cols, rows, groups,
    offsets, node_index, node_table, pole_values, scaling,
    krylov, blocks, previous,
    w_out, p_out, reduced,
    *scratch,
):
    bufs = scratch[:terms]
    (carry, band, prev, image, a_send, a_recv, b_send, b_recv, c_send, c_recv,
     d_send, d_recv, y_send, y_recv, own_sem, band_sem, prev_sem,
     wst, pst, sums, last_sum, basis_sum, part, rs_buf, z_buf, ag_buf,
     w_sem, p_sem, rs_send, rs_recv, z_send, z_recv, ag_send, ag_recv) = scratch[terms:]
    me = lax.axis_index("blk")
    col = lax.axis_index("col")
    core = lax.rem(me, 2)
    chip = lax.div(me, 2)
    par = lax.rem(chip, 2)
    n_chip = n_blk // 2
    n_prev = previous.shape[0]
    partner = (chip + 1 - 2 * par) * 2 + core
    ahead = lax.rem(chip + 2 - 4 * par + n_chip, n_chip) * 2 + core
    sibling = chip * 2 + 1 - core

    def remote(src, dst, send, recv, blk, colpos=None):
        return pltpu.make_async_remote_copy(
            src_ref=src, dst_ref=dst, send_sem=send, recv_sem=recv,
            device_id=(blk, col if colpos is None else colpos), device_id_type=MESH)

    own = [pltpu.make_async_copy(krylov.at[k], bufs[k].at[REACH], own_sem.at[k]) for k in range(terms)]
    band_copy = [pltpu.make_async_copy(blocks.at[0, c], band.at[c], band_sem.at[c]) for c in range(band.shape[0])]
    prev_copy = pltpu.make_async_copy(previous, prev, prev_sem)
    prev_copy.start()

    team, depth = part.shape[0], z_buf.shape[0]
    place = lax.rem(me, 4)
    layer = lax.div(me, 4)
    pos = place * n_col + col

    def member(j):
        other = lax.rem(pos + j, team)
        return other, layer * 4 + lax.div(other, n_col), lax.rem(other, n_col)

    def peer(j):
        return lax.rem(layer + j, depth) * 4 + place

    barrier = pltpu.get_barrier_semaphore()
    for j in range(1, team):
        _, blk, at_col = member(j)
        pl.semaphore_signal(barrier, inc=1, device_id=(blk, at_col), device_id_type=MESH)
    for j in range(1, depth):
        pl.semaphore_signal(barrier, inc=1, device_id=(peer(j), col), device_id_type=MESH)
    pl.semaphore_wait(barrier, team + depth - 2)

    a_copy = [remote(krylov.at[k], bufs[k].at[4 * par], a_send.at[k], a_recv.at[k], partner) for k in range(terms)]
    c_copy = [remote(krylov.at[k], bufs[k].at[1 + 2 * core], c_send.at[k], c_recv.at[k], sibling) for k in range(terms)]
    b_copy = [remote(bufs[k].at[4 - 4 * par], bufs[k].at[4 * par], b_send.at[k], b_recv.at[k], ahead) for k in range(terms)]
    d_copy = [remote(bufs[k].at[4 - 4 * core], bufs[k].at[3 - 2 * core], d_send.at[k], d_recv.at[k], sibling) for k in range(terms)]
    y_copy = remote(krylov.at[terms - 1], carry, y_send, y_recv, me, lax.rem(col + 1, n_col))

    for k in range(terms):
        a_copy[k].start()
    for k in range(terms):
        c_copy[k].start()
    if n_col > 1:
        @pl.when(col < n_col - 1)
        def _():
            y_copy.start()
    for k in range(terms):
        own[k].start()
    for copy in band_copy:
        copy.start()

    @pl.when(col == 0)
    def _():
        carry[...] = jnp.zeros_like(carry)

    w_copy = [pltpu.make_async_copy(wst.at[t], w_out.at[t], w_sem.at[t]) for t in range(terms)]
    p_copy = pltpu.make_async_copy(pst, p_out, p_sem)
    lane = 256

    def arrange(t):
        if t == 0:
            prev_copy.wait()
        p_at = t * 16

        def step(i, _):
            at = pl.ds(pl.multiple_of(i * lane, lane), lane)
            high, low = split(jnp.swapaxes(prev[p_at:p_at + 16, :, at], 0, 1))
            pst[:, p_at:p_at + 16, at] = high
            pst[:, n_prev + p_at:n_prev + p_at + 16, at] = low
            return 0
        lax.fori_loop(0, rows // lane, step, 0)
        if p_at + 16 == n_prev:
            p_copy.start()

    def basis_term(t):
        part = dot_nt(pst[t], pst[t, :n_prev])
        if t == 0:
            basis_sum[...] = part
        else:
            basis_sum[...] += part

    tile = 256
    n_coupling = band.shape[0]

    def ready(group):
        for t in group:
            c_copy[t].wait_recv()
            d_copy[t].wait_recv()
            own[t].wait()
        if group[0] == 0:
            for copy in band_copy:
                copy.wait()

    def image_part(group, start, count):
        picks = [
            jnp.concatenate([bufs[t][offsets[0, c] + REACH] for t in group], axis=0)
            for c in range(n_coupling)
        ]

        def step(i, _):
            at = pl.ds(pl.multiple_of(i * tile, tile), tile)
            total = dot_nt(picks[0], band[0, at, :])
            for c in range(1, n_coupling):
                total = total + dot_nt(picks[c], band[c, at, :])
            image[group[0] * cols:(group[-1] + 1) * cols, at] = total
            return 0
        lax.fori_loop(start, start + count, step, 0)

    def finish(group):
        for t in group:
            shift = jnp.full((8, 128), node_table[node_index[t]], F32)
            weight = jnp.full((8, 128), scaling[t], F32) / (
                1.0 - shift / jnp.full((8, 128), pole_values[t], F32))
            before = carry if t == 0 else bufs[t - 1].at[REACH]
            if t == 0 and n_col > 1:
                @pl.when(col > 0)
                def _():
                    y_copy.wait_recv()
            work = (
                image[t * cols:(t + 1) * cols, :]
                - shift[:1, :1] * bufs[t][REACH].astype(F32)
                + weight[:1, :1] * before[...].astype(F32)
            )
            high, low = split(work)
            wst[t, :cols] = high
            wst[t, cols:] = low
            w_copy[t].start()
            top = dot_nt(pst[t], high)
            self_part = dot_nt(wst[t], high)
            extra = dot_nt(pst[t, :n_prev], low)
            if t == 0:
                sums[:2 * n_prev] = top
                sums[2 * n_prev:] = self_part
                last_sum[...] = extra
            else:
                sums[:2 * n_prev] += top
                sums[2 * n_prev:] += self_part
                last_sum[...] += extra

    n_tiles = rows // tile
    plan = {}
    for j in range(n_prev // 16):
        plan.setdefault(j // 2, []).append(functools.partial(arrange, j))
    for t in range(terms):
        plan.setdefault(-(-n_prev // 32) + t // 3, []).append(functools.partial(basis_term, t))
    first, second, third = groups
    begin = min(terms - 1, first[-1] + 2)
    half = n_tiles // 2
    plan.setdefault(begin, []).extend([
        functools.partial(ready, first), functools.partial(image_part, first, 0, half)])
    plan.setdefault(begin + 1, []).append(functools.partial(image_part, first, half, n_tiles - half))
    plan.setdefault(begin + 2, []).extend([
        functools.partial(finish, first), functools.partial(ready, second),
        functools.partial(image_part, second, 0, half)])
    plan.setdefault(begin + 3, []).extend([
        functools.partial(image_part, second, half, n_tiles - half), functools.partial(finish, second)])

    for k in range(terms + 1):
        if k < terms:
            a_copy[k].wait_recv()
            b_copy[k].start()

            @pl.when(par == core)
            def _():
                d_copy[k].start()
        if k > 0:
            b_copy[k - 1].wait_recv()

            @pl.when(par != core)
            def _():
                d_copy[k - 1].start()
        for item in plan.get(k, ()):
            item()
    ready(third)
    image_part(third, 0, n_tiles)
    finish(third)
    low = sums[2 * n_prev + cols:]
    head = jnp.concatenate([
        sums[:n_prev] + sums[n_prev:2 * n_prev] + last_sum[...],
        sums[2 * n_prev:2 * n_prev + cols] + low + low.T,
    ], axis=1)
    low = basis_sum[n_prev:]
    basis = basis_sum[:n_prev] + low + low.T
    full = jnp.concatenate([head, jnp.concatenate([basis, jnp.zeros_like(basis)], axis=1)], axis=0)
    part[...] = full.reshape(part.shape)
    copies = []
    for j in range(1, team):
        other, blk, at_col = member(j)
        copies.append(remote(part.at[other], rs_buf.at[j - 1], rs_send.at[j - 1], rs_recv.at[j - 1], blk, at_col))
        copies[-1].start()
    total = part[pos]
    for j, copy in enumerate(copies):
        copy.wait_recv()
        total = total + rs_buf[j]
    z_buf[layer] = total
    z_copies = [
        remote(z_buf.at[layer], z_buf.at[layer], z_send.at[j - 1], z_recv.at[j - 1], peer(j))
        for j in range(1, depth)]
    for copy in z_copies:
        copy.start()
    for copy in z_copies:
        copy.wait_recv()
    total = z_buf[0]
    for j in range(1, depth):
        total = total + z_buf[j]
    ag_buf[pos] = total
    ag_copies = []
    for j in range(1, team):
        _, blk, at_col = member(j)
        ag_copies.append(remote(ag_buf.at[pos], ag_buf.at[pos], ag_send.at[j - 1], ag_recv.at[j - 1], blk, at_col))
        ag_copies[-1].start()
    for k in range(terms):
        a_copy[k].wait_send()
        b_copy[k].wait_send()
        c_copy[k].wait_send()
        d_copy[k].wait_send()
        w_copy[k].wait()
    p_copy.wait()
    if n_col > 1:
        @pl.when(col < n_col - 1)
        def _():
            y_copy.wait_send()
    for copy in ag_copies:
        copy.wait_recv()
    reduced[...] = ag_buf[...].reshape(reduced.shape)
    for copy in copies + z_copies + ag_copies:
        copy.wait_send()


def expand(n_blk, n_col, blocks, offsets, krylov, previous, node_table, node_index, pole_values, scaling):
    terms, cols, rows = krylov.shape
    n_prev = previous.shape[0]
    groups = (tuple(range(terms // 2)), tuple(range(terms // 2, 3 * terms // 4)), tuple(range(3 * terms // 4, terms)))
    smem = pl.BlockSpec(memory_space=pltpu.SMEM)
    hbm = pl.BlockSpec(memory_space=pl.ANY)
    vmem = pl.BlockSpec(memory_space=pltpu.VMEM)
    dma = pltpu.SemaphoreType.DMA
    team, depth = 4 * n_col, n_blk // 4
    height = cols + n_prev
    piece = (height // team, 2 * cols)
    return pl.pallas_call(
        functools.partial(expand_kernel, n_blk, n_col, terms, cols, rows, groups),
        out_shape=(
            jax.ShapeDtypeStruct((terms, 2 * cols, rows), BF),
            jax.ShapeDtypeStruct((terms, 2 * n_prev, rows), BF),
            jax.ShapeDtypeStruct((height, 2 * cols), F32),
        ),
        in_specs=[smem] * 5 + [hbm] * 3,
        out_specs=(hbm, hbm, vmem),
        scratch_shapes=[pltpu.VMEM((WIDTH, cols, rows), BF)] * terms + [
            pltpu.VMEM((cols, rows), BF),
            pltpu.VMEM(blocks.shape[1:], BF),
            pltpu.VMEM(previous.shape, F32),
            pltpu.VMEM((terms * cols, rows), F32),
        ] + [dma((terms,))] * 8 + [dma, dma, dma((terms,)), dma((blocks.shape[1],)), dma] + [
            pltpu.VMEM((terms, 2 * cols, rows), BF),
            pltpu.VMEM((terms, 2 * n_prev, rows), BF),
            pltpu.VMEM((2 * n_prev + 2 * cols, cols), F32),
            pltpu.VMEM((n_prev, cols), F32),
            pltpu.VMEM((2 * n_prev, n_prev), F32),
            pltpu.VMEM((team,) + piece, F32),
            pltpu.VMEM((team - 1,) + piece, F32),
            pltpu.VMEM((depth,) + piece, F32),
            pltpu.VMEM((team,) + piece, F32),
            dma((terms,)), dma,
            dma((team - 1,)), dma((team - 1,)),
            dma((depth - 1,)), dma((depth - 1,)),
            dma((team - 1,)), dma((team - 1,)),
        ],
        compiler_params=pltpu.CompilerParams(
            collective_id=0, has_side_effects=True, vmem_limit_bytes=60 * 1024 * 1024),
    )(offsets, node_index, node_table, pole_values, scaling,
      krylov, blocks, previous)


def exact(a, b):
    return jnp.dot(a, b, precision=lax.Precision.HIGHEST, preferred_element_type=F32)


def final_kernel(total_size, reduced, w_in, p_in, out, first, second, factor, stack, result, in_sem, out_sem):
    terms, depth, rows = stack.shape
    cols = first.shape[1]
    n_prev = first.shape[0]
    w_copy = [pltpu.make_async_copy(w_in.at[t], stack.at[t, pl.ds(0, 2 * cols)], in_sem.at[0, t]) for t in range(terms)]
    p_copy = [pltpu.make_async_copy(p_in.at[t], stack.at[t, pl.ds(2 * cols, 2 * n_prev)], in_sem.at[1, t]) for t in range(terms)]
    for t in range(terms):
        w_copy[t].start()
        p_copy[t].start()
    inverse_size = 1.0 / total_size
    root_size = math.sqrt(total_size)
    cross = reduced[:n_prev, :cols] * inverse_size
    self_gram = reduced[:n_prev, cols:] * inverse_size
    basis_gram = reduced[n_prev:, :n_prev] * inverse_size
    coeff_two = cross - exact(basis_gram, cross)
    combined = cross + coeff_two
    turned = combined.T
    mixed = exact(turned, cross)
    gram = self_gram - mixed - mixed.T + exact(turned, exact(basis_gram, combined))
    first[...] = cross * root_size
    second[...] = coeff_two * root_size
    row = lax.broadcasted_iota(jnp.int32, (cols, cols), 0)
    lane = lax.broadcasted_iota(jnp.int32, (cols, cols), 1)
    both = jnp.concatenate([gram, jnp.where(row == lane, 1.0, 0.0)], axis=1)
    below = lax.broadcasted_iota(jnp.int32, (cols, 1), 0)
    for k in range(cols - 1):
        ratio = jnp.where(below > k, both[:, k:k + 1] * (1.0 / both[k:k + 1, k:k + 1]), 0.0)
        both = both - ratio * both[k:k + 1, :]
    left, right = both[:, :cols], both[:, cols:]
    pivots = jnp.sum(jnp.where(row == lane, left, 0.0), axis=1, keepdims=True)
    scale = 1.0 / jnp.sqrt(pivots)
    factor[...] = jnp.where(lane >= row, left * scale, 0.0).T
    inverse = jnp.where(lane <= row, right * scale, 0.0)
    mix = -exact(inverse, turned)
    fh, fl = split(inverse)
    dh, dl = split(mix)
    zero_f, zero_d = jnp.zeros_like(fl), jnp.zeros_like(dl)
    weights = jnp.concatenate([
        jnp.concatenate([fh, fh, dh, dh], axis=1),
        jnp.concatenate([fl, zero_f, dl, zero_d], axis=1),
    ], axis=0)
    out_copy = [pltpu.make_async_copy(result.at[t], out.at[t], out_sem.at[t]) for t in range(terms)]
    for t in range(terms):
        w_copy[t].wait()
        p_copy[t].wait()
        both = jnp.dot(weights, stack[t], preferred_element_type=F32)
        result[t] = (both[:cols] + both[cols:]).astype(BF)
        out_copy[t].start()
    for t in range(terms):
        out_copy[t].wait()


def final(total_size, reduced, wst, pst):
    terms, _, rows = wst.shape
    cols, n_prev = wst.shape[1] // 2, pst.shape[1] // 2
    vmem = pl.BlockSpec(memory_space=pltpu.VMEM)
    hbm = pl.BlockSpec(memory_space=pl.ANY)
    small = jax.ShapeDtypeStruct((n_prev, cols), F32)
    dma = pltpu.SemaphoreType.DMA
    return pl.pallas_call(
        functools.partial(final_kernel, total_size),
        out_shape=(jax.ShapeDtypeStruct((terms, cols, rows), BF), small, small, jax.ShapeDtypeStruct((cols, cols), F32)),
        in_specs=[vmem, hbm, hbm],
        out_specs=(hbm, vmem, vmem, vmem),
        scratch_shapes=[
            pltpu.VMEM((terms, 2 * cols + 2 * n_prev, rows), BF),
            pltpu.VMEM((terms, cols, rows), BF),
            dma((2, terms)), dma((terms,)),
        ],
        compiler_params=pltpu.CompilerParams(vmem_limit_bytes=60 * 1024 * 1024),
    )(reduced, wst, pst)


def body(n_blk, n_col, blocks, offsets, krylov, previous, node_table, node_index, pole_values, scaling):
    terms, cols, rows = krylov.shape
    wst, pst, reduced = expand(
        n_blk, n_col, blocks, offsets, krylov, previous, node_table, node_index, pole_values, scaling)
    return final(rows * n_blk * terms * n_col, reduced, wst, pst)


def solution(mesh):
    in_specs = (
        P("blk", None, None, None),
        P("blk", None),
        P("col", None, "blk"),
        P(None, "col", "blk"),
        P(),
        P("col"),
        P("col"),
        P("col"),
    )
    out_specs = (P("col", None, "blk"), P(), P(), P())
    call = functools.partial(body, mesh.shape["blk"], mesh.shape["col"])
    return jax.shard_map(call, mesh=mesh, in_specs=in_specs, out_specs=out_specs, check_vma=False)
```
